32 devices in a mesh: seq: 16 (over z, y, x), fsdp: 2 (over core).
Axes of the slice: x: 2, y: 2, z: 4, core: 2. Of those that a mesh axis runs over, the one named last changes fastest.
Arguments:
- tokens: bfloat16 [2, 12288, 2560], P('fsdp', 'seq'), may hold values from -6 to 6
- bounds: int32 [2, 16, 2], P('fsdp', 'seq'), may hold values from 0 to 24, as said below
- in_weight: bfloat16 [2560, 5416], P(('seq', 'fsdp')), may hold values from -0.125 to 0.125
- conv_weight: float32 [4, 2816], replicated, may hold values from -0.6 to 0.6
- conv_bias: float32 [2816], replicated, may hold values from -3 to 3
- dt_bias: float32 [40], replicated, may hold values from -4 to 0
- decay_rate: float32 [40], replicated, may hold values from 4.8828125e-05 to 0.5
- skip_gain: float32 [40], replicated, may hold values from 0.1 to 1.9
- norm_gain: float32 [2560], replicated, may hold values from 0.1 to 1.9
Outputs:
- layer_out: bfloat16 [2, 12288, 2560], P('fsdp', 'seq')
The draws below stay inside these ranges and needn't reach their ends.
Inputs may be any that keep to these rules, and one draw needn't show every extreme that they name: For sequence b, bounds[b, s] holds the first and one past the last block of the shard of index s of seq; shards are consecutive in s and cover all 24 blocks; each holds 1 to 3 blocks, and some shard holds 3.
All inputs are finite; a program needn't handle non-finite values.
Results may differ from the reference program's by a relative error of at most 0.0028.
The reference program's roundings to bfloat16 on the way count: a program that leaves them out, or rounds other values in their place, can miss the bound.
Values may be sent and summed in bfloat16 or wider, within the bound.
A program may use at most 192 MiB of HBM per device.

```python
import jax
import jax.numpy as jnp
from jax import lax

D = 2560
HEADS = 40
HEAD_DIM = 64
STATE = 128
CONV = 4
BLOCK = 256
SLOT_BLOCKS = 3
INNER = 2560
COLS = 5416
SLOTS = 768
TOTAL_BLOCKS = 24
SEQ_LEN = 6144
SEQS = 2
N_SEQ = 16


def draw_bounds(key, part):
    rows = []
    for index in range(SEQS):
        subkey = jax.random.fold_in(key, 11 + index)
        pick_key, order_key = jax.random.split(subkey)
        heavy = jax.random.randint(pick_key, (), 1, N_SEQ // 4 + 1)
        middle = N_SEQ // 2 - 2 * heavy
        ranking = jax.random.permutation(order_key, N_SEQ)
        counts = jnp.where(ranking < heavy, 3, jnp.where(ranking < heavy + middle, 2, 1)).astype(jnp.int32)
        ends = jnp.cumsum(counts).astype(jnp.int32)
        rows.append(jnp.stack([ends - counts, ends], axis=1))
    return jnp.stack(rows).astype(jnp.int32)


def draw_decay_rate(key, part):
    choose_key, value_key = jax.random.split(jax.random.fold_in(key, 5))
    slow_heads = jax.random.uniform(choose_key, (HEADS,)) < 0.5
    spread = jax.random.uniform(value_key, (HEADS,), jnp.float32)
    slow_rate = 0.3 / SEQ_LEN * jnp.exp(spread * jnp.log(10.0))
    fast_rate = 0.05 * jnp.exp(spread * jnp.log(10.0))
    return jnp.where(slow_heads, slow_rate, fast_rate).astype(jnp.float32)


def levels(rng, shape, shards, low, largest):
    gain = 1.0
    for position, shards_of in shards:
        draws = jax.random.uniform(jax.random.fold_in(jax.random.fold_in(rng, 6), position), (shards_of,), jnp.float32, low / len(shards), largest / len(shards))
        gain = gain * jnp.repeat(jnp.exp(draws), shape[position] // shards_of).reshape((-1,) + (1,) * (len(shape) - 1 - position))
    return gain


def noise(stream_key, shape, scale, limit, cuts=(), dtype=jnp.bfloat16):
    array = scale * jax.random.normal(stream_key, shape, jnp.float32)
    if cuts:
        array = array * levels(stream_key, shape, cuts, -0.22, 0.18)
    return jnp.clip(array, -limit, limit).astype(dtype)


def setup_inputs(seed: int = 0) -> dict:
    arg_keys = jax.random.split(jax.random.key(seed), 10)
    tokens = noise(arg_keys[0], (SEQS, N_SEQ * SLOTS, D), 1.0, 6.0, ((0, 2), (1, 16)))
    bounds = draw_bounds(jax.random.fold_in(arg_keys[9], 71), 0)
    in_weight = noise(arg_keys[2], (D, COLS), D ** -0.5, 0.125, ((0, 32),))
    conv_weight = jnp.clip(jax.random.uniform(arg_keys[3], (CONV, INNER + 2 * STATE), jnp.float32, -0.6, 0.6), -0.6, 0.6)
    conv_bias = noise(arg_keys[4], (INNER + 2 * STATE,), 0.5, 3.0, (), jnp.float32)
    dt_bias = jnp.clip(jax.random.uniform(arg_keys[5], (HEADS,), jnp.float32, -4.0, 0.0), -4.0, 0.0)
    decay_rate = draw_decay_rate(jax.random.fold_in(arg_keys[9], 71), 0)
    skip_gain = jnp.clip(1.0 + 0.18 * jax.random.normal(arg_keys[7], (HEADS,), jnp.float32), 0.1, 1.9)
    norm_gain = jnp.clip(1.0 + 0.18 * jax.random.normal(arg_keys[8], (INNER,), jnp.float32), 0.1, 1.9)
    return dict(tokens=tokens, bounds=bounds, in_weight=in_weight, conv_weight=conv_weight, conv_bias=conv_bias, dt_bias=dt_bias, decay_rate=decay_rate, skip_gain=skip_gain, norm_gain=norm_gain)


def block_terms(head_input, input_map, output_map, step_size, decay_rate):
    log_decay = -(step_size * decay_rate[None, :]).T
    cumulative = jnp.cumsum(log_decay, axis=1)
    pairwise = cumulative[:, :, None] - cumulative[:, None, :]
    length = cumulative.shape[1]
    causal = jnp.arange(length)[:, None] >= jnp.arange(length)[None, :]
    pair_decay = jnp.exp(jnp.where(causal[None], pairwise, -jnp.inf))
    scores = jnp.dot(output_map, input_map.T, preferred_element_type=jnp.float32)
    mixing = scores[None] * pair_decay * step_size.T[:, None, :]
    inner_out = jnp.einsum('hij,jhp->ihp', mixing, head_input, precision=lax.Precision.HIGH)
    to_end = jnp.exp(cumulative[:, -1:] - cumulative) * step_size.T
    local_state = jnp.einsum('hj,jhp,jn->hpn', to_end, head_input, input_map.astype(jnp.float32), precision=lax.Precision.HIGH)
    return (inner_out, cumulative, local_state)

def carried(output_map, cumulative, state):
    reach = jnp.einsum('in,hpn->ihp', output_map.astype(jnp.float32), state, precision=lax.Precision.HIGH)
    return jnp.exp(cumulative).T[:, :, None] * reach

def one_sequence(tokens, bounds, in_weight, conv_weight, conv_bias, dt_bias, decay_rate, skip_gain, norm_gain):
    starts = bounds[:, 0]
    ends = bounds[:, 1]
    blocks = jnp.arange(TOTAL_BLOCKS).astype(jnp.int32)
    owner = lax.optimization_barrier(jnp.sum((ends[None, :] <= blocks[:, None]).astype(jnp.int32), axis=1)).astype(jnp.int32)
    slot_row = (owner * SLOT_BLOCKS + blocks - starts[owner]).astype(jnp.int32)
    grouped = tokens.reshape(N_SEQ * SLOT_BLOCKS, BLOCK, D)
    live = grouped[slot_row].reshape(SEQ_LEN, D)
    projected = jnp.dot(live, in_weight, preferred_element_type=jnp.float32).astype(jnp.bfloat16)
    gate = projected[:, :INNER].astype(jnp.float32)
    mixed_in = projected[:, INNER:2 * INNER + 2 * STATE]
    raw_step = projected[:, 2 * INNER + 2 * STATE:].astype(jnp.float32)
    padded = jnp.concatenate([jnp.zeros((CONV - 1, mixed_in.shape[1]), jnp.bfloat16), mixed_in], axis=0)
    convolved = jnp.zeros((SEQ_LEN, mixed_in.shape[1]), jnp.float32) + conv_bias[None, :]
    for offset in range(CONV):
        convolved = convolved + conv_weight[offset][None, :] * padded[offset:offset + SEQ_LEN].astype(jnp.float32)
    conv_out = jax.nn.silu(convolved).astype(jnp.bfloat16)
    head_input = conv_out[:, :INNER].astype(jnp.float32).reshape(TOTAL_BLOCKS, BLOCK, HEADS, HEAD_DIM)
    input_map = conv_out[:, INNER:INNER + STATE].reshape(TOTAL_BLOCKS, BLOCK, STATE)
    output_map = conv_out[:, INNER + STATE:].reshape(TOTAL_BLOCKS, BLOCK, STATE)
    step_size = jax.nn.softplus(raw_step + dt_bias[None, :]).reshape(TOTAL_BLOCKS, BLOCK, HEADS)

    def advance(state, pieces):
        in_values, in_map, out_map, in_step = pieces
        inner_out, cumulative, local_state = block_terms(in_values, in_map, out_map, in_step, decay_rate)
        result = inner_out + carried(out_map, cumulative, state) + skip_gain[None, :, None] * in_values
        state = jnp.exp(cumulative[:, -1])[:, None, None] * state + local_state
        return (state, result)
    initial = jnp.zeros((HEADS, HEAD_DIM, STATE), jnp.float32)
    final_state, outputs = lax.scan(advance, initial, (head_input, input_map, output_map, step_size))
    scanned = outputs.reshape(SEQ_LEN, INNER)
    gated = scanned * jax.nn.silu(gate)
    normed = gated * lax.rsqrt(lax.optimization_barrier(jnp.mean(gated * gated, axis=1, keepdims=True)) + 1e-05) * norm_gain[None, :]
    placed = jnp.zeros((N_SEQ * SLOT_BLOCKS, BLOCK, INNER), jnp.bfloat16)
    placed = placed.at[slot_row].set(normed.astype(jnp.bfloat16).reshape(TOTAL_BLOCKS, BLOCK, INNER))
    return placed.reshape(N_SEQ * SLOTS, INNER)

def reference(tokens, bounds, in_weight, conv_weight, conv_bias, dt_bias, decay_rate, skip_gain, norm_gain):
    results = [one_sequence(tokens[index], bounds[index], in_weight, conv_weight, conv_bias, dt_bias, decay_rate, skip_gain, norm_gain) for index in range(SEQS)]
    return jnp.stack(results)
```

```python
import jax
import jax.numpy as jnp
from jax import lax
from jax.experimental import pallas as pl
from jax.sharding import PartitionSpec as P

BLOCK = 256


def passed_along(value, axis, steps):
    count = lax.axis_size(axis)
    leading, last = (max(0, -steps), min(count, count - steps))
    return lax.ppermute(value, axis, [(source, source + steps) for source in range(leading, last)])


def compose_kernel(state_ref, decay_ref, before_ref):
    def one(turn, state):
        before_ref[turn] = state
        return decay_ref[turn] * state + state_ref[turn]

    lax.fori_loop(0, state_ref.shape[0], one, jnp.zeros(state_ref.shape[1:], jnp.float32))


def carried_in(decay_total, summary_state, axis):
    count = lax.axis_size(axis)
    heads, head_dim, width = summary_state.shape
    share = heads * head_dim // count
    extra = -(-share // width)
    decay_rows = jnp.repeat(decay_total, head_dim).reshape(count, share)
    decay_rows = jnp.pad(decay_rows, ((0, 0), (0, extra * width - share)))
    sent = jnp.concatenate(
        [summary_state.reshape(count, share, width), decay_rows.reshape(count, extra, width)], axis=1
    )
    got = lax.all_to_all(sent, axis, 0, 0)
    decays = got[:, share:].reshape(count, extra * width)[:, :share, None]
    before = pl.pallas_call(
        compose_kernel,
        out_shape=jax.ShapeDtypeStruct((count, share, width), jnp.float32),
        cost_estimate=pl.CostEstimate(flops=1000000, bytes_accessed=4000000, transcendentals=0),
    )(got[:, :share], decays)
    return lax.all_to_all(before, axis, 0, 0).reshape(heads, head_dim, width)


def block_terms(head_input, input_map, output_map, step_size, decay_rate):
    log_decay = -(step_size * decay_rate[None, :]).T
    cumulative = jnp.cumsum(log_decay, axis=1)
    pairwise = cumulative[:, :, None] - cumulative[:, None, :]
    length = cumulative.shape[1]
    causal = jnp.arange(length)[:, None] >= jnp.arange(length)[None, :]
    pair_decay = jnp.exp(jnp.where(causal[None], pairwise, -jnp.inf))
    scores = jnp.dot(output_map, input_map.T, preferred_element_type=jnp.float32)
    mixing = scores[None] * pair_decay * step_size.T[:, None, :]
    inner_out = jnp.einsum("hij,jhp->ihp", mixing, head_input, precision=lax.Precision.HIGH)
    to_end = jnp.exp(cumulative[:, -1:] - cumulative) * step_size.T
    local_state = jnp.einsum(
        "hj,jhp,jn->hpn",
        to_end,
        head_input,
        input_map.astype(jnp.float32),
        precision=lax.Precision.HIGH,
    )
    return (inner_out, cumulative, local_state)


def carried(output_map, cumulative, state):
    reach = jnp.einsum(
        "in,hpn->ihp", output_map.astype(jnp.float32), state, precision=lax.Precision.HIGH
    )
    return jnp.exp(cumulative).T[:, :, None] * reach


def local(
    tokens, bounds, in_weight, conv_weight, conv_bias, dt_bias, decay_rate, skip_gain, norm_gain
):
    slots = tokens.shape[1]
    inner = norm_gain.shape[0]
    state_width = (conv_bias.shape[0] - inner) // 2
    heads = decay_rate.shape[0]
    head_dim = inner // heads
    kernel = conv_weight.shape[0]
    capacity = slots // BLOCK
    shard_blocks = bounds[0, 0, 1] - bounds[0, 0, 0]
    own_rows = tokens[0]
    every = ("seq", "fsdp")
    mixed_weight = lax.all_gather(in_weight[:, inner:], every, axis=0, tiled=True)
    gate_share, mixed_weight = lax.optimization_barrier((in_weight[:, :inner], mixed_weight))
    gate_weight = lax.all_gather(gate_share, every, axis=0, tiled=True)
    projected = jnp.dot(own_rows, mixed_weight, preferred_element_type=jnp.float32).astype(
        jnp.bfloat16
    )
    mixed_in = projected[:, : inner + 2 * state_width]
    raw_step = projected[:, inner + 2 * state_width :].astype(jnp.float32)
    edge_rows = lax.dynamic_slice_in_dim(
        mixed_in, shard_blocks * BLOCK - (kernel - 1), kernel - 1, 0
    )
    previous = passed_along(edge_rows, "seq", 1)
    extended = jnp.concatenate([previous, mixed_in], axis=0)
    convolved = jnp.zeros((slots, mixed_in.shape[1]), jnp.float32) + conv_bias[None, :]
    for offset in range(kernel):
        convolved = convolved + conv_weight[offset][None, :] * extended[
            offset : offset + slots
        ].astype(jnp.float32)
    conv_out = jax.nn.silu(convolved).astype(jnp.bfloat16)
    live_mask = jnp.arange(slots)[:, None] < shard_blocks * BLOCK
    step_size = jnp.where(live_mask, jax.nn.softplus(raw_step + dt_bias[None, :]), 0.0)
    pieces = []
    decay_total = jnp.ones((heads,), jnp.float32)
    summary_state = jnp.zeros((heads, head_dim, state_width), jnp.float32)
    for place in range(capacity):
        lower = place * BLOCK
        upper = lower + BLOCK
        in_values = (
            conv_out[lower:upper, :inner].astype(jnp.float32).reshape(BLOCK, heads, head_dim)
        )
        in_map = conv_out[lower:upper, inner : inner + state_width]
        out_map = conv_out[lower:upper, inner + state_width :]
        inner_out, cumulative, local_state = block_terms(
            in_values, in_map, out_map, step_size[lower:upper], decay_rate
        )
        block_decay = jnp.exp(cumulative[:, -1])
        summary_state = block_decay[:, None, None] * summary_state + local_state
        decay_total = decay_total * block_decay
        pieces.append((in_values, out_map, inner_out, cumulative, local_state, block_decay))
    state = carried_in(decay_total, summary_state, "seq")
    gate = lax.reduce_precision(
        jnp.dot(own_rows, gate_weight, preferred_element_type=jnp.float32), 8, 7
    )
    results = []
    for in_values, out_map, inner_out, cumulative, local_state, block_decay in pieces:
        result = (
            inner_out + carried(out_map, cumulative, state) + skip_gain[None, :, None] * in_values
        )
        results.append(result.reshape(BLOCK, inner))
        state = block_decay[:, None, None] * state + local_state
    scanned = jnp.concatenate(results, axis=0)
    gated = scanned * jax.nn.silu(gate)
    normed = (
        gated
        * lax.rsqrt(jnp.mean(gated * gated, axis=1, keepdims=True) + 1e-05)
        * norm_gain[None, :]
    )
    layer_out = jnp.where(live_mask, normed, 0.0).astype(jnp.bfloat16)
    return layer_out[None]


def solution(mesh):
    in_specs = (
        P("fsdp", "seq", None),
        P("fsdp", "seq", None),
        P(("seq", "fsdp"), None),
        P(),
        P(),
        P(),
        P(),
        P(),
        P(),
    )
    out_specs = P("fsdp", "seq", None)
    return jax.shard_map(local, mesh=mesh, in_specs=in_specs, out_specs=out_specs, check_vma=False)
```
